512 devices in a mesh: ens: 2 (over y), bfly: 32 (over z), cblk: 8 (over x, core).
Axes of the slice: x: 4, y: 2, z: 32, core: 2. Of those that a mesh axis runs over, the one named last changes fastest.
The devices are a block of a 4x8x32 slice.
Arguments:
- source: bfloat16 [1048576, 512], P(('ens', 'bfly', 'cblk')), parts along dimension 0, may hold values from -6 to 6
- basis: bfloat16 [1048576, 256], P(('ens', 'bfly', 'cblk')), parts along dimension 0, may hold values from -0.046875 to 0.046875
- transfer: bfloat16 [10, 32, 256, 512], P('ens', 'bfly'), parts along dimension 0, may hold values from -0.25 to 0.25
- skeleton: int32 [512, 16], P(('ens', 'bfly', 'cblk')), parts along dimension 0, may hold values from 0 to 15, each once within a row
- row_class: int32 [1048576], P(('ens', 'bfly', 'cblk')), parts along dimension 0, may hold values from 0 to 15
- linear_table: float32 [16, 512], replicated, may hold values from 0.5 to 1.5
- cubic_table: float32 [16, 512], replicated, may hold values from 0.05 to 0.3
Outputs:
- adjoint: bfloat16 [1048576, 512], P(('ens', 'bfly', 'cblk')), parts along dimension 0
The draws below stay inside these ranges and needn't reach their ends.
There are 2 independent parts, one for each index of `ens`. The reference program is written for one: setup_inputs(seed, part) draws one part's arguments, and reference() takes and returns one part's arrays. A program takes and returns all parts, laid end to end along the dimension named above; an argument that names none is the same for every part. Nothing has to cross between parts.
Inputs may be any that keep to these rules, and one draw needn't show every extreme that they name: Each row of skeleton names each of the 16 tiles once.
All inputs are finite; a program needn't handle non-finite values.
Results may differ from the reference program's by a relative error of at most 0.0052.
Values may be sent and summed in bfloat16 or wider, within the bound.
No kernel may reach another device: no remote copies, remote signals or barrier semaphores. Data moves between devices by JAX's collectives and lax.ppermute only.
A program may use at most 64 MiB of HBM per device.

```python
import math
import jax
import jax.numpy as jnp
import numpy as np
from jax import lax

R = 256
C = 512
TILE = 128
KTAB = 16
TILES = 16
ROWS_BLK = 16384
ROWS = 524288
LEVELS = 5
N_BFLY = 32
N_CBLK = 8


def with_ends(result, rng, low, high):
    longest = result.shape.index(max(result.shape))
    spots = []
    for shift in (0, 1):
        where = [jax.random.randint(jax.random.fold_in(rng, axis), (), 0, length) for axis, length in enumerate(result.shape)]
        where[longest] = (where[longest] + shift) % result.shape[longest]
        spots.append(tuple(where))
    return result.at[spots[0]].set(low).at[spots[1]].set(high)


def block_levels(own_key, shape, cuts, low, top_value):
    level, own = 1.0, jax.random.fold_in(own_key, 6)
    for axis_at, blocks in cuts:
        steps = jnp.exp(jax.random.uniform(jax.random.fold_in(own, axis_at), (blocks,), jnp.float32, low / len(cuts), top_value / len(cuts)))
        level = level * jnp.repeat(steps, shape[axis_at] // blocks).reshape([-1 if axis == axis_at else 1 for axis in range(len(shape))])
    return level


def normal_values(rng, extent, width, reach, pieces=(), dtype=jnp.bfloat16):
    values = width * jax.random.normal(rng, extent, jnp.float32)
    if pieces:
        values = values * block_levels(rng, extent, pieces, -0.22, 0.18)
    return jnp.clip(values, -reach, reach).astype(dtype)


def setup_inputs(seed: int = 0, part: int = 0) -> dict:
    streams_of = jax.random.split(jax.random.key(seed), 8)
    part_splits = jax.random.split(jax.random.fold_in(streams_of[7], part), 8)
    return {
        "source": normal_values(part_splits[0], (ROWS, C), 1.0, 6.0, ((0, 256),)),
        "basis": normal_values(part_splits[1], (ROWS, R), ROWS_BLK ** -0.5, 0.046875, ((0, 256),)),
        "transfer": normal_values(part_splits[2], (LEVELS, N_BFLY, R, 2 * R), (2 * R) ** -0.5, 0.25, ((1, 32),)),
        "skeleton": jax.vmap(lambda own: jax.random.permutation(own, TILES))(jax.random.split(part_splits[3], (N_BFLY * N_CBLK))).reshape((N_BFLY * N_CBLK, TILES)).astype(jnp.int32),
        "row_class": with_ends(jax.random.randint(part_splits[4], (ROWS,), 0, KTAB), jax.random.fold_in(part_splits[4], 1), 0, KTAB - 1).astype(jnp.int32),
        "linear_table": jnp.clip(jax.random.uniform(streams_of[5], (KTAB, C), jnp.float32, 0.5, 1.5), 0.5, 1.5),
        "cubic_table": jnp.clip(jax.random.uniform(streams_of[6], (KTAB, C), jnp.float32, 0.05, 0.3), 0.05, 0.3),
    }


def reference(source, basis, transfer, skeleton, row_class, linear_table, cubic_table):
    highest = lax.Precision.HIGHEST
    blocks = N_BFLY
    devices = N_BFLY * N_CBLK
    tiled = source.reshape(devices, TILES, TILE, C)
    picked = jnp.take_along_axis(tiled, skeleton.astype(jnp.int32)[:, :, None, None], axis=1)
    picked = picked.reshape(blocks, ROWS_BLK, C).astype(jnp.float32)
    leaves = basis.reshape(blocks, ROWS_BLK, R).astype(jnp.float32)
    coefficient = jnp.einsum('bmr,bmc->brc', leaves, picked, precision=highest)
    factors = transfer.astype(jnp.float32)
    first = factors[:, :, :, :R]
    second = factors[:, :, :, R:]
    for level in range(LEVELS):
        partner = np.arange(blocks) ^ 1 << level
        coefficient = jnp.einsum('bij,bjc->bic', first[level], coefficient, precision=highest) + jnp.einsum('bij,bjc->bic', second[level], coefficient[partner], precision=highest)
    carried = coefficient.astype(jnp.bfloat16)
    factor_rho = math.sqrt(ROWS_BLK / R)
    mapped = factor_rho * jnp.einsum('bmr,brc->bmc', leaves, carried.astype(jnp.float32), precision=highest)
    mapped = mapped.reshape(ROWS, C)
    linear = linear_table[row_class]
    cubic = cubic_table[row_class]
    weighted = (mapped * (linear + cubic * mapped * mapped)).astype(jnp.bfloat16)
    weighted = weighted.reshape(blocks, ROWS_BLK, C).astype(jnp.float32)
    back = jnp.einsum('bmr,bmc->brc', leaves, weighted, precision=highest)
    for level in reversed(range(LEVELS)):
        partner = np.arange(blocks) ^ 1 << level
        sending = jnp.einsum('bji,bjc->bic', second[level], back, precision=highest)
        back = jnp.einsum('bji,bjc->bic', first[level], back, precision=highest) + sending[partner]
    returned = back.astype(jnp.bfloat16)
    ordered = (factor_rho * jnp.einsum('bmr,brc->bmc', leaves, returned.astype(jnp.float32), precision=highest)).astype(jnp.bfloat16)
    ordered = ordered.reshape(devices, TILES, TILE, C)
    inverse = jnp.argsort(skeleton, axis=1).astype(jnp.int32)
    adjoint = jnp.take_along_axis(ordered, inverse[:, :, None, None], axis=1)
    return adjoint.reshape(ROWS, C)
```

```python
import math

import jax
import jax.numpy as jnp
from jax import lax
from jax.experimental import pallas as pl
from jax.experimental.pallas import tpu as pltpu
from jax.sharding import PartitionSpec as P

F32 = jnp.float32
BF16 = jnp.bfloat16
VMEM_LIMIT = 24 * 1024 * 1024


def vmem():
    return pl.BlockSpec(memory_space=pltpu.VMEM)


def smem():
    return pl.BlockSpec(memory_space=pltpu.SMEM)


def cost(flops, bytes_accessed):
    return pl.CostEstimate(flops=flops, bytes_accessed=bytes_accessed, transcendentals=0)


def dot(left, right, left_dim, right_dim):
    return lax.dot_general(
        left, right, (((left_dim,), (right_dim,)), ((), ())), preferred_element_type=F32
    )


def leaf_kernel(order_ref, source_ref, basis_ref, out_ref, acc_ref):
    tiles = order_ref.shape[1]
    tile = source_ref.shape[0] // tiles
    step = 4
    for start in range(0, tiles, step):
        picked = jnp.concatenate(
            [
                source_ref[pl.ds(pl.multiple_of(order_ref[0, start + i] * tile, tile), tile), :]
                for i in range(step)
            ],
            axis=0,
        )
        term = dot(picked, basis_ref[pl.ds(start * tile, step * tile), :], 0, 0)
        if start == 0:
            acc_ref[...] = term
        elif start + step < tiles:
            acc_ref[...] += term
        else:
            out_ref[...] = (acc_ref[...] + term).astype(out_ref.dtype)


def leaf_terms(source, basis, skeleton):
    rows, columns = source.shape
    rank = basis.shape[1]
    return pl.pallas_call(
        leaf_kernel,
        name="leaf",
        out_shape=jax.ShapeDtypeStruct((columns, rank), BF16),
        in_specs=[smem(), vmem(), vmem()],
        out_specs=vmem(),
        scratch_shapes=[pltpu.VMEM((columns, rank), F32)],
        compiler_params=pltpu.CompilerParams(vmem_limit_bytes=VMEM_LIMIT),
        cost_estimate=cost(2 * rows * columns * rank, 2 * rows * (columns + rank)),
    )(skeleton, source, basis)


def in_three(table):
    high = table.astype(BF16)
    rest = table - high.astype(F32)
    middle = rest.astype(BF16)
    low = (rest - middle.astype(F32)).astype(BF16)
    return jnp.concatenate([high.astype(F32), middle.astype(F32), low.astype(F32)], axis=0)


def middle_kernel(
    factor_rho, carried_ref, basis_ref, class_ref, linear_ref, cubic_ref, out_ref, acc_ref
):
    rows = basis_ref.shape[0]
    classes = linear_ref.shape[0]
    linear_parts = in_three(linear_ref[...]).T.astype(BF16)
    cubic_parts = in_three(cubic_ref[...]).T.astype(BF16)
    step = 256
    for start in range(0, rows, step):
        basis = basis_ref[pl.ds(start, step), :]
        mapped = factor_rho * dot(carried_ref[...], basis, 1, 1)
        ids = lax.broadcasted_iota(jnp.int32, (classes, step), 0)
        hot = (ids == class_ref[:, pl.ds(start, step)]).astype(F32)
        hot = jnp.concatenate([hot, hot, hot], axis=0).astype(BF16)
        linear = dot(linear_parts, hot, 1, 0)
        cubic = dot(cubic_parts, hot, 1, 0)
        weighted = (mapped * (linear + cubic * mapped * mapped)).astype(BF16)
        term = dot(weighted, basis, 1, 0)
        if start == 0:
            acc_ref[...] = term
        elif start + step < rows:
            acc_ref[...] += term
        else:
            out_ref[...] = (acc_ref[...] + term).astype(out_ref.dtype)


def middle(carried, basis, row_class, linear_table, cubic_table, factor_rho):
    columns, rank = carried.shape
    rows = basis.shape[0]

    def body(*refs):
        middle_kernel(factor_rho, *refs)

    return pl.pallas_call(
        body,
        name="middle",
        out_shape=jax.ShapeDtypeStruct((columns, rank), BF16),
        in_specs=[vmem()] * 5,
        out_specs=vmem(),
        scratch_shapes=[pltpu.VMEM((columns, rank), F32)],
        compiler_params=pltpu.CompilerParams(vmem_limit_bytes=VMEM_LIMIT),
        cost_estimate=cost(8 * rows * columns * rank, 2 * rows * rank),
    )(carried, basis, row_class.reshape(1, rows), linear_table, cubic_table)


def expand_kernel(factor_rho, order_ref, returned_ref, basis_ref, out_ref, held_ref, sems):
    tiles = order_ref.shape[1]
    tile = basis_ref.shape[0] // tiles
    step = 4
    copies = []
    for start in range(0, tiles, step):
        part = factor_rho * dot(
            basis_ref[pl.ds(start * tile, step * tile), :], returned_ref[...], 1, 1
        )
        held_ref[pl.ds(start * tile, step * tile), :] = part.astype(held_ref.dtype)
        for i in range(start, start + step):
            place = pl.multiple_of(order_ref[0, i] * tile, tile)
            copies.append(
                pltpu.make_async_copy(
                    held_ref.at[pl.ds(i * tile, tile), :],
                    out_ref.at[pl.ds(place, tile), :],
                    sems.at[i],
                )
            )
            copies[-1].start()
    for copy in copies:
        copy.wait()


def expand_rows(returned, basis, skeleton, factor_rho):
    columns, rank = returned.shape
    rows = basis.shape[0]
    tiles = skeleton.shape[1]

    def body(*refs):
        expand_kernel(factor_rho, *refs)

    return pl.pallas_call(
        body,
        name="expand",
        out_shape=jax.ShapeDtypeStruct((rows, columns), BF16),
        in_specs=[smem(), vmem(), vmem()],
        out_specs=pl.BlockSpec(memory_space=pltpu.HBM),
        scratch_shapes=[pltpu.VMEM((rows, columns), BF16), pltpu.SemaphoreType.DMA((tiles,))],
        compiler_params=pltpu.CompilerParams(vmem_limit_bytes=VMEM_LIMIT),
        cost_estimate=cost(2 * rows * columns * rank, 2 * rows * (columns + rank)),
    )(skeleton, returned, basis)


def from_partner(array, axis, bit):
    return lax.ppermute(array, axis, [(i, i ^ 1 << bit) for i in range(lax.axis_size(axis))])


def sum_at_owner(array, axis):
    count = lax.axis_size(axis)
    blocks = array.reshape(count, array.shape[0] // count, array.shape[1])
    arrived = lax.all_to_all(blocks, axis, split_axis=0, concat_axis=0, tiled=True)
    return arrived.astype(F32).sum(axis=0)


def from_everyone(array, axis):
    copies = jnp.broadcast_to(array, (lax.axis_size(axis), *array.shape))
    arrived = lax.all_to_all(copies, axis, split_axis=0, concat_axis=0, tiled=True)
    return arrived.reshape(-1, array.shape[1])


def times(left, right, right_dim):
    if left.dtype == BF16:
        return dot(left, right, 1, right_dim)
    return lax.dot_general(
        left,
        right.astype(F32),
        (((1,), (right_dim,)), ((), ())),
        precision=lax.Precision.HIGHEST,
        preferred_element_type=F32,
    )


def sent(array, level):
    return array.astype(BF16) if level >= 3 else array


def forward_levels(coefficient, factors):
    rank = factors.shape[1]
    for level in range(factors.shape[0]):
        partner = from_partner(sent(coefficient, level), "bfly", level)
        coefficient = times(coefficient, factors[level, :, :rank], 1) + times(
            partner, factors[level, :, rank:], 1
        )
    return coefficient


def adjoint_levels(coefficient, factors):
    rank = factors.shape[1]
    for level in reversed(range(factors.shape[0])):
        sending = times(coefficient, factors[level, :, rank:], 0)
        received = from_partner(sent(sending, level), "bfly", level)
        coefficient = times(coefficient, factors[level, :, :rank], 0) + received.astype(F32)
    return coefficient


def per_device(source, basis, transfer, skeleton, row_class, linear_table, cubic_table):
    factors = transfer[:, 0]
    factor_rho = math.sqrt(source.shape[0] * lax.axis_size("cblk") / basis.shape[1])
    summed = sum_at_owner(leaf_terms(source, basis, skeleton), "cblk")
    carried = forward_levels(summed, factors).astype(BF16)
    back = middle(
        from_everyone(carried, "cblk"), basis, row_class, linear_table, cubic_table, factor_rho
    )
    returned = adjoint_levels(sum_at_owner(back, "cblk"), factors).astype(BF16)
    return expand_rows(from_everyone(returned, "cblk"), basis, skeleton, factor_rho)


def solution(mesh):
    placed = (
        P(("ens", "bfly", "cblk"), None),
        P(("ens", "bfly", "cblk"), None),
        P("ens", "bfly", None, None),
        P(("ens", "bfly", "cblk"), None),
        P(("ens", "bfly", "cblk")),
        P(),
        P(),
    )
    return jax.shard_map(
        per_device,
        mesh=mesh,
        in_specs=placed,
        out_specs=P(("ens", "bfly", "cblk"), None),
        check_vma=False,
    )
```

```python
import math

import jax
import jax.numpy as jnp
from jax import lax
from jax.experimental import pallas as pl
from jax.experimental.pallas import tpu as pltpu
from jax.sharding import PartitionSpec as P


F32 = jnp.float32
BF16 = jnp.bfloat16
VMEM_LIMIT = 24 * 1024 * 1024


def vmem():
    return pl.BlockSpec(memory_space=pltpu.VMEM)


def hbm():
    return pl.BlockSpec(memory_space=pltpu.HBM)


def smem():
    return pl.BlockSpec(memory_space=pltpu.SMEM)


def cost(flops, bytes_accessed):
    return pl.CostEstimate(flops=flops, bytes_accessed=bytes_accessed, transcendentals=0)


def dot(left, right, left_dim, right_dim):
    return lax.dot_general(
        left, right, (((left_dim,), (right_dim,)), ((), ())), preferred_element_type=F32
    )


def leaf_kernel(order_ref, source_ref, basis_ref, out_ref, acc_ref):
    tiles = order_ref.shape[1]
    tile = source_ref.shape[0] // tiles
    step = 4
    for start in range(0, tiles, step):
        picked = jnp.concatenate(
            [
                source_ref[pl.ds(pl.multiple_of(order_ref[0, start + i] * tile, tile), tile), :]
                for i in range(step)
            ],
            axis=0,
        )
        term = dot(picked, basis_ref[pl.ds(start * tile, step * tile), :], 0, 0)
        if start == 0:
            acc_ref[...] = term
        elif start + step < tiles:
            acc_ref[...] += term
        else:
            out_ref[...] = (acc_ref[...] + term).astype(out_ref.dtype)


def leaf_terms(source, basis, skeleton):
    rows, columns = source.shape
    rank = basis.shape[1]
    return pl.pallas_call(
        leaf_kernel,
        name="leaf",
        out_shape=jax.ShapeDtypeStruct((columns, rank), BF16),
        in_specs=[smem(), vmem(), vmem()],
        out_specs=vmem(),
        scratch_shapes=[pltpu.VMEM((columns, rank), F32)],
        compiler_params=pltpu.CompilerParams(vmem_limit_bytes=VMEM_LIMIT),
        cost_estimate=cost(2 * rows * columns * rank, 2 * rows * (columns + rank)),
    )(skeleton, source, basis)


def product(left, right, right_dim):
    rows = left.shape[0]
    high = left.astype(BF16)
    low = (left - high.astype(F32)).astype(BF16)
    both = dot(jnp.concatenate([high, low], axis=0), right, 1, right_dim)
    return both[:rows] + both[rows:]


def factor(factors_ref, level, part):
    rank = factors_ref.shape[1]
    return factors_ref[level, :, part * rank : (part + 1) * rank]


def in_group():
    return lax.rem(lax.axis_index("bfly"), 4)


def spread(send_ref, first, second, third):
    place = in_group()
    send_ref[place] = first.astype(send_ref.dtype)
    send_ref[place ^ 1] = first.astype(send_ref.dtype)
    send_ref[place ^ 2] = second.astype(send_ref.dtype)
    send_ref[place ^ 3] = third.astype(send_ref.dtype)


def sum_kernel(arrived_ref, out_ref):
    out_ref[...] = jnp.sum(arrived_ref[...].astype(F32), axis=0)


def up_send_kernel(summed_ref, factors_ref, extra_ref, send_ref, own_ref):
    del extra_ref
    summed = summed_ref[...]
    own = product(summed, factor(factors_ref, 0, 0), 1)
    own_ref[...] = own
    spread(send_ref, summed, own, summed)


def up_take_kernel(own_ref, arrived_ref, factors_ref, extra_ref, out_ref):
    place = in_group()
    near = own_ref[...] + dot(arrived_ref[place ^ 1], factor(factors_ref, 0, 1), 1, 1)
    far = arrived_ref[place ^ 2].astype(F32) + dot(arrived_ref[place ^ 3], extra_ref[...], 1, 1)
    out_ref[...] = product(near, factor(factors_ref, 1, 0), 1) + product(
        far, factor(factors_ref, 1, 1), 1
    )


def down_send_kernel(value_ref, factors_ref, extra_ref, send_ref, own_ref):
    value = value_ref[...]
    own = product(value, factor(factors_ref, 1, 0), 0)
    far = product(value, factor(factors_ref, 1, 1), 0)
    own_ref[...] = own
    spread(
        send_ref,
        product(own, factor(factors_ref, 0, 1), 0),
        far,
        product(far, extra_ref[...], 0),
    )


def down_take_kernel(own_ref, arrived_ref, factors_ref, out_ref):
    place = in_group()
    total = product(
        own_ref[...] + arrived_ref[place ^ 2].astype(F32), factor(factors_ref, 0, 0), 0
    )
    total += arrived_ref[place ^ 1].astype(F32) + arrived_ref[place ^ 3].astype(F32)
    out_ref[...] = jnp.broadcast_to(total.astype(out_ref.dtype), out_ref.shape)


def small_call(body, out_shape, *args):
    return pl.pallas_call(
        body,
        out_shape=out_shape,
        in_specs=[vmem()] * len(args),
        out_specs=jax.tree.map(lambda _: vmem(), out_shape),
        compiler_params=pltpu.CompilerParams(vmem_limit_bytes=VMEM_LIMIT),
        cost_estimate=cost(1 << 27, 1 << 20),
    )(*args)


def in_fours(array):
    size = lax.axis_size("bfly")
    groups = [list(range(start, start + 4)) for start in range(0, size, 4)]
    return lax.all_to_all(
        array, "bfly", split_axis=0, concat_axis=0, axis_index_groups=groups, tiled=True
    )


def in_three(table):
    high = table.astype(BF16)
    rest = table - high.astype(F32)
    middle = rest.astype(BF16)
    low = (rest - middle.astype(F32)).astype(BF16)
    return jnp.concatenate([high.astype(F32), middle.astype(F32), low.astype(F32)], axis=0)


def middle_kernel(
    factor_rho, carried_ref, basis_ref, class_ref, linear_ref, cubic_ref, out_ref, acc_ref
):
    rows = basis_ref.shape[0]
    classes = linear_ref.shape[0]
    linear_parts = in_three(linear_ref[...]).T.astype(BF16)
    cubic_parts = in_three(cubic_ref[...]).T.astype(BF16)
    step = 256
    for start in range(0, rows, step):
        basis = basis_ref[pl.ds(start, step), :]
        mapped = factor_rho * dot(carried_ref[...], basis, 1, 1)
        ids = lax.broadcasted_iota(jnp.int32, (classes, step), 0)
        hot = (ids == class_ref[:, pl.ds(start, step)]).astype(F32)
        hot = jnp.concatenate([hot, hot, hot], axis=0).astype(BF16)
        linear = dot(linear_parts, hot, 1, 0)
        cubic = dot(cubic_parts, hot, 1, 0)
        weighted = (mapped * (linear + cubic * mapped * mapped)).astype(BF16)
        term = dot(weighted, basis, 1, 0)
        if start == 0:
            acc_ref[...] = term
        elif start + step < rows:
            acc_ref[...] += term
        else:
            out_ref[...] = (acc_ref[...] + term).astype(out_ref.dtype)


def middle(carried, basis, row_class, linear_table, cubic_table, factor_rho):
    columns, rank = carried.shape
    rows = basis.shape[0]

    def body(*refs):
        middle_kernel(factor_rho, *refs)

    return pl.pallas_call(
        body,
        name="middle",
        out_shape=jax.ShapeDtypeStruct((columns, rank), BF16),
        in_specs=[vmem()] * 5,
        out_specs=vmem(),
        scratch_shapes=[pltpu.VMEM((columns, rank), F32)],
        compiler_params=pltpu.CompilerParams(vmem_limit_bytes=VMEM_LIMIT),
        cost_estimate=cost(8 * rows * columns * rank, 2 * rows * rank),
    )(carried, basis, row_class.reshape(1, rows), linear_table, cubic_table)


def expand_kernel(factor_rho, order_ref, returned_ref, basis_ref, out_ref, held_ref, sems):
    tiles = order_ref.shape[1]
    tile = basis_ref.shape[0] // tiles
    step = 4
    copies = []
    for start in range(0, tiles, step):
        part = factor_rho * dot(
            basis_ref[pl.ds(start * tile, step * tile), :], returned_ref[...], 1, 1
        )
        held_ref[pl.ds(start * tile, step * tile), :] = part.astype(held_ref.dtype)
        for i in range(start, start + step):
            place = pl.multiple_of(order_ref[0, i] * tile, tile)
            copies.append(
                pltpu.make_async_copy(
                    held_ref.at[pl.ds(i * tile, tile), :],
                    out_ref.at[pl.ds(place, tile), :],
                    sems.at[i],
                )
            )
            copies[-1].start()
    for copy in copies:
        copy.wait()


def expand_rows(returned, basis, skeleton, factor_rho):
    columns, rank = returned.shape
    rows = basis.shape[0]
    tiles = skeleton.shape[1]

    def body(*refs):
        expand_kernel(factor_rho, *refs)

    return pl.pallas_call(
        body,
        name="expand",
        out_shape=jax.ShapeDtypeStruct((rows, columns), BF16),
        in_specs=[smem(), vmem(), vmem()],
        out_specs=hbm(),
        scratch_shapes=[pltpu.VMEM((rows, columns), BF16), pltpu.SemaphoreType.DMA((tiles,))],
        compiler_params=pltpu.CompilerParams(vmem_limit_bytes=VMEM_LIMIT),
        cost_estimate=cost(2 * rows * columns * rank, 2 * rows * (columns + rank)),
    )(skeleton, returned, basis)


def from_partner(array, axis, bit):
    return lax.ppermute(array, axis, [(i, i ^ 1 << bit) for i in range(lax.axis_size(axis))])


def shared_out(array, axis):
    count = lax.axis_size(axis)
    blocks = array.reshape(count, array.shape[0] // count, array.shape[1])
    return lax.all_to_all(blocks, axis, split_axis=0, concat_axis=0, tiled=True)


def times(left, right, right_dim):
    if left.dtype == BF16:
        return dot(left, right, 1, right_dim)
    return lax.dot_general(
        left,
        right.astype(F32),
        (((1,), (right_dim,)), ((), ())),
        precision=lax.Precision.HIGHEST,
        preferred_element_type=F32,
    )


def sent(array, level):
    return array.astype(BF16) if level >= 3 else array


def forward_levels(coefficient, factors):
    rank = factors.shape[1]
    for level in range(2, factors.shape[0]):
        partner = from_partner(sent(coefficient, level), "bfly", level)
        coefficient = times(coefficient, factors[level, :, :rank], 1) + times(
            partner, factors[level, :, rank:], 1
        )
    return coefficient


def adjoint_levels(coefficient, factors):
    rank = factors.shape[1]
    for level in reversed(range(2, factors.shape[0])):
        sending = times(coefficient, factors[level, :, rank:], 0)
        received = from_partner(sent(sending, level), "bfly", level)
        coefficient = times(coefficient, factors[level, :, :rank], 0) + received.astype(F32)
    return coefficient


def per_device(source, basis, transfer, skeleton, row_class, linear_table, cubic_table):
    factors = transfer[:, 0]
    rank = basis.shape[1]
    shares = lax.axis_size("cblk")
    factor_rho = math.sqrt(source.shape[0] * shares / rank)
    extra = from_partner(factors[0, :, rank:], "bfly", 1)
    leaves = leaf_terms(source, basis, skeleton)
    leaves = shared_out(leaves, "cblk")
    columns = leaves.shape[1]
    whole = jax.ShapeDtypeStruct((columns, rank), F32)
    fours = jax.ShapeDtypeStruct((4, columns, rank), BF16)
    eights = jax.ShapeDtypeStruct((shares, columns, rank), BF16)

    summed = small_call(sum_kernel, whole, leaves)
    send, own = small_call(up_send_kernel, (fours, whole), summed, factors, extra)
    low = small_call(up_take_kernel, whole, own, in_fours(send), factors, extra)
    carried = forward_levels(low, factors).astype(BF16)
    carried = shared_out(
        jnp.broadcast_to(carried, eights.shape).reshape(shares * columns, rank), "cblk"
    ).reshape(shares * columns, rank)
    back = middle(carried, basis, row_class, linear_table, cubic_table, factor_rho)
    summed = shared_out(back, "cblk").astype(F32).sum(axis=0)
    high = adjoint_levels(summed, factors)
    send, own = small_call(down_send_kernel, (fours, whole), high, factors, extra)
    returned = small_call(down_take_kernel, eights, own, in_fours(send), factors)
    returned = lax.all_to_all(returned, "cblk", split_axis=0, concat_axis=0, tiled=True)
    return expand_rows(returned.reshape(shares * columns, rank), basis, skeleton, factor_rho)


def solution(mesh):
    placed = (
        P(("ens", "bfly", "cblk"), None),
        P(("ens", "bfly", "cblk"), None),
        P("ens", "bfly", None, None),
        P(("ens", "bfly", "cblk"), None),
        P(("ens", "bfly", "cblk")),
        P(),
        P(),
    )

    return jax.shard_map(
        per_device,
        mesh=mesh,
        in_specs=placed,
        out_specs=P(("ens", "bfly", "cblk"), None),
        check_vma=False,
    )
```

```python
import math

import jax
import jax.numpy as jnp
from jax import lax
from jax.experimental import pallas as pl
from jax.experimental.pallas import tpu as pltpu
from jax.sharding import PartitionSpec as P


F32 = jnp.float32
BF16 = jnp.bfloat16
VMEM_LIMIT = 24 * 1024 * 1024
LEAF_LIMIT = 66_200_000
LABEL_ROWS = 16


def vmem():
    return pl.BlockSpec(memory_space=pltpu.VMEM)


def hbm():
    return pl.BlockSpec(memory_space=pltpu.HBM)


def smem():
    return pl.BlockSpec(memory_space=pltpu.SMEM)


def cost(flops, bytes_accessed):
    return pl.CostEstimate(flops=flops, bytes_accessed=bytes_accessed, transcendentals=0)


def dot(left, right, left_dim, right_dim):
    return lax.dot_general(
        left, right, (((left_dim,), (right_dim,)), ((), ())), preferred_element_type=F32
    )


def leaf_kernel(
    order_hbm,
    class_hbm,
    source_hbm,
    basis_hbm,
    out_ref,
    packed_hbm,
    acc_ref,
    order_ref,
    class_ref,
    source_ref,
    basis_ref,
    label_ref,
    sems,
):
    rows = source_ref.shape[0]
    basis_in = pltpu.make_async_copy(basis_hbm, basis_ref, sems.at[0])
    source_in = pltpu.make_async_copy(source_hbm, source_ref, sems.at[1])
    order_in = pltpu.make_async_copy(order_hbm, order_ref, sems.at[2])
    class_in = pltpu.make_async_copy(class_hbm, class_ref, sems.at[3])
    for copy in (order_in, class_in, basis_in, source_in):
        copy.start()
    class_in.wait()
    width = label_ref.shape[1]
    label = [class_ref[:, pl.ds(at, width)].astype(F32) for at in range(0, rows, width)]
    label.append(jnp.zeros((label_ref.shape[0] - len(label), width), F32))
    label_ref[...] = jnp.concatenate(label, axis=0).astype(label_ref.dtype)
    basis_in.wait()
    basis_out = pltpu.make_async_copy(basis_ref, packed_hbm.at[pl.ds(0, rows), :], sems.at[4])
    basis_out.start()
    order_in.wait()
    source_in.wait()
    label_out = pltpu.make_async_copy(
        label_ref, packed_hbm.at[pl.ds(rows, label_ref.shape[0]), :], sems.at[5]
    )
    label_out.start()
    tiles = order_ref.shape[1]
    tile = rows // tiles
    step = 4
    for start in range(0, tiles, step):
        picked = jnp.concatenate(
            [
                source_ref[pl.ds(pl.multiple_of(order_ref[0, start + i] * tile, tile), tile), :]
                for i in range(step)
            ],
            axis=0,
        )
        term = dot(picked, basis_ref[pl.ds(start * tile, step * tile), :], 0, 0)
        if start == 0:
            acc_ref[...] = term
        elif start + step < tiles:
            acc_ref[...] += term
        else:
            out_ref[...] = (acc_ref[...] + term).astype(out_ref.dtype)
    basis_out.wait()
    label_out.wait()


def leaf_terms(source, basis, skeleton, row_class):
    rows, columns = source.shape
    rank = basis.shape[1]
    labels = LABEL_ROWS
    return pl.pallas_call(
        leaf_kernel,
        name="leaf",
        out_shape=(
            jax.ShapeDtypeStruct((columns, rank), BF16),
            jax.ShapeDtypeStruct((rows + labels, rank), BF16),
        ),
        in_specs=[hbm()] * 4,
        out_specs=(vmem(), hbm()),
        scratch_shapes=[
            pltpu.VMEM((columns, rank), F32),
            pltpu.SMEM(skeleton.shape, jnp.int32),
            pltpu.VMEM((1, rows), jnp.int32),
            pltpu.VMEM(source.shape, source.dtype),
            pltpu.VMEM(basis.shape, basis.dtype),
            pltpu.VMEM((labels, rank), BF16),
            pltpu.SemaphoreType.DMA((6,)),
        ],
        compiler_params=pltpu.CompilerParams(vmem_limit_bytes=LEAF_LIMIT),
        cost_estimate=cost(2 * rows * columns * rank, 2 * rows * (columns + rank)),
    )(skeleton, row_class.reshape(1, rows), source, basis)


def product(left, right, right_dim):
    rows = left.shape[0]
    high = left.astype(BF16)
    low = (left - high.astype(F32)).astype(BF16)
    both = dot(jnp.concatenate([high, low], axis=0), right, 1, right_dim)
    return both[:rows] + both[rows:]


def factor(factors_ref, level, part):
    rank = factors_ref.shape[1]
    return factors_ref[level, :, part * rank : (part + 1) * rank]


def in_group():
    return lax.rem(lax.axis_index("bfly"), 4)


def spread(send_ref, first, second, third):
    place = in_group()
    send_ref[place] = first.astype(send_ref.dtype)
    send_ref[place ^ 1] = first.astype(send_ref.dtype)
    send_ref[place ^ 2] = second.astype(send_ref.dtype)
    send_ref[place ^ 3] = third.astype(send_ref.dtype)


def down_send_kernel(value_ref, factors_ref, extra_ref, send_ref, own_ref):
    value = value_ref[...]
    own = product(value, factor(factors_ref, 1, 0), 0)
    far = product(value, factor(factors_ref, 1, 1), 0)
    own_ref[...] = own
    spread(
        send_ref,
        product(own, factor(factors_ref, 0, 1), 0),
        far,
        product(far, extra_ref[...], 0),
    )


def down_take_kernel(own_ref, arrived_ref, factors_ref, out_ref):
    place = in_group()
    total = product(
        own_ref[...] + arrived_ref[place ^ 2].astype(F32), factor(factors_ref, 0, 0), 0
    )
    total += arrived_ref[place ^ 1].astype(F32) + arrived_ref[place ^ 3].astype(F32)
    out_ref[...] = jnp.broadcast_to(total.astype(out_ref.dtype), out_ref.shape)


def small_call(body, out_shape, *args):
    return pl.pallas_call(
        body,
        out_shape=out_shape,
        in_specs=[vmem()] * len(args),
        out_specs=jax.tree.map(lambda _: vmem(), out_shape),
        compiler_params=pltpu.CompilerParams(vmem_limit_bytes=VMEM_LIMIT),
        cost_estimate=cost(1 << 27, 1 << 20),
    )(*args)


def in_fours(array):
    size = lax.axis_size("bfly")
    groups = [list(range(start, start + 4)) for start in range(0, size, 4)]
    return lax.all_to_all(
        array, "bfly", split_axis=0, concat_axis=0, axis_index_groups=groups, tiled=True
    )


def in_three(table):
    high = table.astype(BF16)
    rest = table - high.astype(F32)
    middle = rest.astype(BF16)
    low = (rest - middle.astype(F32)).astype(BF16)
    return jnp.concatenate([high.astype(F32), middle.astype(F32), low.astype(F32)], axis=0)


def middle_kernel(factor_rho, count, *refs):
    carried_ref, linear_ref, cubic_ref = refs[:3]
    packed = refs[3 : 3 + count]
    out_ref, table_ref, held_ref, sems = refs[3 + count :]
    copies = [
        pltpu.make_async_copy(packed[at], held_ref.at[at], sems.at[at]) for at in range(count)
    ]
    for copy in copies:
        copy.start()
    columns = carried_ref.shape[0]
    classes = linear_ref.shape[0]
    rows = held_ref.shape[1] - LABEL_ROWS
    width = held_ref.shape[2]
    share = pl.ds(pl.multiple_of(lax.axis_index("cblk") * columns, columns), columns)
    table_ref[0] = in_three(linear_ref[...]).T
    table_ref[1] = in_three(cubic_ref[...]).T
    tables = jnp.concatenate([table_ref[0, share, :], table_ref[1, share, :]], axis=0).astype(BF16)
    step = 2 * width
    ids = lax.broadcasted_iota(jnp.int32, (classes, step), 0).astype(F32)
    total = jnp.zeros((columns, width), F32)
    for at in range(count):
        copies[at].wait()
        labels = held_ref[at, pl.ds(rows, LABEL_ROWS), :].astype(F32)
        for start in range(0, rows, step):
            basis = held_ref[at, pl.ds(start, step), :]
            mapped = factor_rho * dot(carried_ref[...], basis, 1, 1)
            first = start // width
            label = jnp.concatenate([labels[first : first + 1], labels[first + 1 : first + 2]], axis=1)
            hot = (ids == label).astype(F32)
            hot = jnp.concatenate([hot, hot, hot], axis=0).astype(BF16)
            looked = dot(tables, hot, 1, 0)
            weighted = mapped * (looked[:columns] + looked[columns:] * mapped * mapped)
            total += dot(weighted.astype(BF16), basis, 1, 0)
    out_ref[...] = total


def middle(carried, packed, linear_table, cubic_table, factor_rho):
    columns, rank = carried.shape
    count = len(packed)
    tall = packed[0].shape[0]

    def body(*refs):
        middle_kernel(factor_rho, count, *refs)

    return pl.pallas_call(
        body,
        name="middle",
        out_shape=jax.ShapeDtypeStruct((columns, rank), F32),
        in_specs=[vmem()] * 3 + [pl.BlockSpec(memory_space=pl.ANY)] * count,
        out_specs=vmem(),
        scratch_shapes=[
            pltpu.VMEM((2, linear_table.shape[1], 3 * linear_table.shape[0]), F32),
            pltpu.VMEM((count, tall, rank), BF16),
            pltpu.SemaphoreType.DMA((count,)),
        ],
        compiler_params=pltpu.CompilerParams(vmem_limit_bytes=VMEM_LIMIT),
        cost_estimate=cost(8 * count * tall * columns * rank, 2 * count * tall * rank),
    )(carried, linear_table, cubic_table, *packed)


def expand_kernel(factor_rho, order_ref, returned_ref, basis_ref, out_ref, held_ref, sems):
    tiles = order_ref.shape[1]
    tile = basis_ref.shape[0] // tiles
    step = 4
    copies = []
    for start in range(0, tiles, step):
        part = factor_rho * dot(
            basis_ref[pl.ds(start * tile, step * tile), :], returned_ref[...], 1, 1
        )
        held_ref[pl.ds(start * tile, step * tile), :] = part.astype(held_ref.dtype)
        for i in range(start, start + step):
            place = pl.multiple_of(order_ref[0, i] * tile, tile)
            copies.append(
                pltpu.make_async_copy(
                    held_ref.at[pl.ds(i * tile, tile), :],
                    out_ref.at[pl.ds(place, tile), :],
                    sems.at[i],
                )
            )
            copies[-1].start()
    for copy in copies:
        copy.wait()


def expand_rows(returned, basis, skeleton, factor_rho):
    columns, rank = returned.shape
    rows = basis.shape[0]
    tiles = skeleton.shape[1]

    def body(*refs):
        expand_kernel(factor_rho, *refs)

    return pl.pallas_call(
        body,
        name="expand",
        out_shape=jax.ShapeDtypeStruct((rows, columns), BF16),
        in_specs=[smem(), vmem(), vmem()],
        out_specs=hbm(),
        scratch_shapes=[pltpu.VMEM((rows, columns), BF16), pltpu.SemaphoreType.DMA((tiles,))],
        compiler_params=pltpu.CompilerParams(vmem_limit_bytes=VMEM_LIMIT),
        cost_estimate=cost(2 * rows * columns * rank, 2 * rows * (columns + rank)),
    )(skeleton, returned, basis)


def from_partner(array, axis, bit):
    return lax.ppermute(array, axis, [(i, i ^ 1 << bit) for i in range(lax.axis_size(axis))])


def shared_out(array, axis):
    count = lax.axis_size(axis)
    blocks = array.reshape(count, array.shape[0] // count, array.shape[1])
    return lax.all_to_all(blocks, axis, split_axis=0, concat_axis=0, tiled=True)


def times(left, right, right_dim):
    if left.dtype == BF16:
        return dot(left, right, 1, right_dim)
    return lax.dot_general(
        left,
        right.astype(F32),
        (((1,), (right_dim,)), ((), ())),
        precision=lax.Precision.HIGHEST,
        preferred_element_type=F32,
    )


def sent(array, level):
    return array.astype(BF16) if level >= 3 else array


def forward_levels(coefficient, factors):
    rank = factors.shape[1]
    for level in range(factors.shape[0]):
        partner = from_partner(sent(coefficient, level), "bfly", level)
        coefficient = times(coefficient, factors[level, :, :rank], 1) + times(
            partner, factors[level, :, rank:], 1
        )
    return coefficient


def adjoint_levels(coefficient, factors):
    rank = factors.shape[1]
    for level in reversed(range(2, factors.shape[0])):
        sending = times(coefficient, factors[level, :, rank:], 0)
        received = from_partner(sent(sending, level), "bfly", level)
        coefficient = times(coefficient, factors[level, :, :rank], 0) + received.astype(F32)
    return coefficient


def swapped(array, mask):
    return lax.ppermute(array, "cblk", [(i, i ^ mask) for i in range(lax.axis_size("cblk"))])


def per_device(source, basis, transfer, skeleton, row_class, linear_table, cubic_table):
    factors = transfer[:, 0]
    rank = basis.shape[1]
    shares = lax.axis_size("cblk")
    factor_rho = math.sqrt(source.shape[0] * shares / rank)
    leaves, packed = leaf_terms(source, basis, skeleton, row_class)
    leaves = shared_out(leaves, "cblk")
    columns = leaves.shape[1]
    whole = jax.ShapeDtypeStruct((columns, rank), F32)
    fours = jax.ShapeDtypeStruct((4, columns, rank), BF16)
    eights = jax.ShapeDtypeStruct((shares, columns, rank), BF16)

    far = [swapped(packed, mask) for mask in range(2, shares, 2)]
    near = [swapped(packed, 1)]
    near += [swapped(array, 1) for array in far]
    extra = from_partner(factors[0, :, rank:], "bfly", 1)

    carried = forward_levels(leaves.astype(F32).sum(axis=0), factors).astype(BF16)
    back = middle(carried, [packed, *far, *near], linear_table, cubic_table, factor_rho)
    high = adjoint_levels(back, factors)
    send, own = small_call(down_send_kernel, (fours, whole), high, factors, extra)
    returned = small_call(down_take_kernel, eights, own, in_fours(send), factors)
    returned = lax.all_to_all(returned, "cblk", split_axis=0, concat_axis=0, tiled=True)
    return expand_rows(returned.reshape(shares * columns, rank), basis, skeleton, factor_rho)


def solution(mesh):
    placed = (
        P(("ens", "bfly", "cblk"), None),
        P(("ens", "bfly", "cblk"), None),
        P("ens", "bfly", None, None),
        P(("ens", "bfly", "cblk"), None),
        P(("ens", "bfly", "cblk")),
        P(),
        P(),
    )

    return jax.shard_map(
        per_device,
        mesh=mesh,
        in_specs=placed,
        out_specs=P(("ens", "bfly", "cblk"), None),
        check_vma=False,
    )
```

```python
import math

import jax
import jax.numpy as jnp
from jax import lax
from jax.experimental import pallas as pl
from jax.experimental.pallas import tpu as pltpu
from jax.sharding import PartitionSpec as P


F32 = jnp.float32
BF16 = jnp.bfloat16
VMEM_LIMIT = 24 * 1024 * 1024
LEAF_LIMIT = 65600000
LABEL_ROWS = 16


def vmem():
    return pl.BlockSpec(memory_space=pltpu.VMEM)


def hbm():
    return pl.BlockSpec(memory_space=pltpu.HBM)


def smem():
    return pl.BlockSpec(memory_space=pltpu.SMEM)


def cost(flops, bytes_accessed):
    return pl.CostEstimate(flops=flops, bytes_accessed=bytes_accessed, transcendentals=0)


def dot(left, right, left_dim, right_dim):
    return lax.dot_general(
        left, right, (((left_dim,), (right_dim,)), ((), ())), preferred_element_type=F32
    )


def leaf_kernel(
    order_hbm,
    class_hbm,
    source_hbm,
    basis_hbm,
    out_ref,
    packed_hbm,
    acc_ref,
    order_ref,
    place_ref,
    class_ref,
    source_ref,
    basis_ref,
    label_ref,
    sems,
    source_sems,
):
    rows = source_ref.shape[0]
    tiles = order_ref.shape[1]
    tile = rows // tiles
    step = 4
    order_in = pltpu.make_async_copy(order_hbm, order_ref, sems.at[0])
    basis_in = pltpu.make_async_copy(basis_hbm, basis_ref, sems.at[1])
    source_in = [
        pltpu.make_async_copy(
            source_hbm.at[pl.ds(at * tile, step * tile), :],
            source_ref.at[pl.ds(at * tile, step * tile), :],
            source_sems.at[at // step],
        )
        for at in range(0, tiles, step)
    ]
    class_in = pltpu.make_async_copy(class_hbm, class_ref, sems.at[2])
    for copy in (order_in, basis_in, *source_in, class_in):
        copy.start()
    order_in.wait()
    for i in range(tiles):
        place_ref[order_ref[0, i]] = i
    basis_in.wait()
    basis_out = pltpu.make_async_copy(basis_ref, packed_hbm.at[pl.ds(0, rows), :], sems.at[3])
    basis_out.start()
    for start in range(0, tiles, step):
        source_in[start // step].wait()
        matched = jnp.concatenate(
            [
                basis_ref[pl.ds(pl.multiple_of(place_ref[start + i] * tile, tile), tile), :]
                for i in range(step)
            ],
            axis=0,
        )
        term = dot(source_ref[pl.ds(start * tile, step * tile), :], matched, 0, 0)
        if start == 0:
            acc_ref[...] = term
        elif start + step < tiles:
            acc_ref[...] += term
        else:
            out_ref[...] = (acc_ref[...] + term).astype(out_ref.dtype)
        if start == 0:
            class_in.wait()
            width = label_ref.shape[1]
            label = [class_ref[:, pl.ds(at, width)].astype(F32) for at in range(0, rows, width)]
            label.append(jnp.zeros((label_ref.shape[0] - len(label), width), F32))
            label_ref[...] = jnp.concatenate(label, axis=0).astype(label_ref.dtype)
        elif start == step:
            label_out = pltpu.make_async_copy(
                label_ref, packed_hbm.at[pl.ds(rows, label_ref.shape[0]), :], sems.at[4]
            )
            label_out.start()
    basis_out.wait()
    label_out.wait()


def leaf_terms(source, basis, skeleton, row_class):
    rows, columns = source.shape
    rank = basis.shape[1]
    labels = LABEL_ROWS
    return pl.pallas_call(
        leaf_kernel,
        name="leaf",
        out_shape=(
            jax.ShapeDtypeStruct((columns, rank), BF16),
            jax.ShapeDtypeStruct((rows + labels, rank), BF16),
        ),
        in_specs=[hbm()] * 4,
        out_specs=(vmem(), hbm()),
        scratch_shapes=[
            pltpu.VMEM((columns, rank), F32),
            pltpu.SMEM(skeleton.shape, jnp.int32),
            pltpu.SMEM((skeleton.shape[1],), jnp.int32),
            pltpu.VMEM((1, rows), jnp.int32),
            pltpu.VMEM(source.shape, source.dtype),
            pltpu.VMEM(basis.shape, basis.dtype),
            pltpu.VMEM((labels, rank), BF16),
            pltpu.SemaphoreType.DMA((5,)),
            pltpu.SemaphoreType.DMA((skeleton.shape[1] // 4,)),
        ],
        compiler_params=pltpu.CompilerParams(vmem_limit_bytes=LEAF_LIMIT),
        cost_estimate=cost(2 * rows * columns * rank, 2 * rows * (columns + rank)),
    )(skeleton, row_class.reshape(1, rows), source, basis)


def product(left, right, right_dim):
    rows = left.shape[0]
    high = left.astype(BF16)
    low = (left - high.astype(F32)).astype(BF16)
    both = dot(jnp.concatenate([high, low], axis=0), right, 1, right_dim)
    return both[:rows] + both[rows:]


def factor(factors_ref, level, part):
    rank = factors_ref.shape[1]
    return factors_ref[level, :, part * rank : (part + 1) * rank]


def in_group():
    return lax.rem(lax.axis_index("bfly"), 4)


def spread(send_ref, first, second, third):
    place = in_group()
    send_ref[place] = first.astype(send_ref.dtype)
    send_ref[place ^ 1] = first.astype(send_ref.dtype)
    send_ref[place ^ 2] = second.astype(send_ref.dtype)
    send_ref[place ^ 3] = third.astype(send_ref.dtype)


def down_send_kernel(value_ref, factors_ref, extra_ref, send_ref, own_ref):
    value = value_ref[...]
    own = product(value, factor(factors_ref, 1, 0), 0)
    far = product(value, factor(factors_ref, 1, 1), 0)
    own_ref[...] = own
    spread(
        send_ref,
        product(own, factor(factors_ref, 0, 1), 0),
        far,
        product(far, extra_ref[...], 0),
    )


def down_take_kernel(own_ref, arrived_ref, factors_ref, out_ref):
    place = in_group()
    total = product(
        own_ref[...] + arrived_ref[place ^ 2].astype(F32), factor(factors_ref, 0, 0), 0
    )
    total += arrived_ref[place ^ 1].astype(F32) + arrived_ref[place ^ 3].astype(F32)
    out_ref[...] = jnp.broadcast_to(total.astype(out_ref.dtype), out_ref.shape)


def small_call(body, out_shape, *args):
    return pl.pallas_call(
        body,
        out_shape=out_shape,
        in_specs=[vmem()] * len(args),
        out_specs=jax.tree.map(lambda _: vmem(), out_shape),
        compiler_params=pltpu.CompilerParams(vmem_limit_bytes=VMEM_LIMIT),
        cost_estimate=cost(1 << 27, 1 << 20),
    )(*args)


def in_fours(array):
    size = lax.axis_size("bfly")
    groups = [list(range(start, start + 4)) for start in range(0, size, 4)]
    return lax.all_to_all(
        array, "bfly", split_axis=0, concat_axis=0, axis_index_groups=groups, tiled=True
    )


def in_three(table):
    high = table.astype(BF16)
    rest = table - high.astype(F32)
    middle = rest.astype(BF16)
    low = (rest - middle.astype(F32)).astype(BF16)
    return jnp.concatenate([high.astype(F32), middle.astype(F32), low.astype(F32)], axis=0)


def middle_kernel(factor_rho, count, *refs):
    carried_ref, linear_ref, cubic_ref = refs[:3]
    packed = refs[3 : 3 + count]
    out_ref, table_ref = refs[3 + count :]
    columns = carried_ref.shape[0]
    classes = linear_ref.shape[0]
    rows = packed[0].shape[0] - LABEL_ROWS
    width = packed[0].shape[1]
    lanes = table_ref.shape[1]
    shares = lanes // columns
    mine = lax.axis_index("cblk")
    wide = pl.ds(pl.multiple_of(mine // shares * lanes, lanes), lanes)
    share = pl.ds(pl.multiple_of(lax.rem(mine, shares) * columns, columns), columns)
    table_ref[0] = in_three(linear_ref[:, wide]).T
    table_ref[1] = in_three(cubic_ref[:, wide]).T
    tables = jnp.concatenate([table_ref[0, share, :], table_ref[1, share, :]], axis=0).astype(BF16)
    step = 2 * width
    ids = lax.broadcasted_iota(jnp.int32, (classes, step), 0).astype(F32)
    total = jnp.zeros((columns, width), F32)
    for ref in packed:
        labels = ref[pl.ds(rows, LABEL_ROWS), :].astype(F32)
        for start in range(0, rows, step):
            basis = ref[pl.ds(start, step), :]
            mapped = factor_rho * dot(carried_ref[...], basis, 1, 1)
            first = start // width
            label = jnp.concatenate([labels[first : first + 1], labels[first + 1 : first + 2]], axis=1)
            hot = (ids == label).astype(F32)
            hot = jnp.concatenate([hot, hot, hot], axis=0).astype(BF16)
            looked = dot(tables, hot, 1, 0)
            weighted = mapped * (looked[:columns] + looked[columns:] * mapped * mapped)
            total += dot(weighted.astype(BF16), basis, 1, 0)
    out_ref[...] = total


def middle(carried, packed, linear_table, cubic_table, factor_rho):
    columns, rank = carried.shape
    count = len(packed)
    tall = packed[0].shape[0]

    def body(*refs):
        middle_kernel(factor_rho, count, *refs)

    return pl.pallas_call(
        body,
        name="middle",
        out_shape=jax.ShapeDtypeStruct((columns, rank), F32),
        in_specs=[vmem()] * (3 + count),
        out_specs=vmem(),
        scratch_shapes=[pltpu.VMEM((2, max(columns, 128), 3 * linear_table.shape[0]), F32)],
        compiler_params=pltpu.CompilerParams(vmem_limit_bytes=VMEM_LIMIT),
        cost_estimate=cost(8 * count * tall * columns * rank, 2 * count * tall * rank),
    )(carried, linear_table, cubic_table, *packed)


def expand_kernel(factor_rho, order_ref, returned_ref, basis_ref, out_ref, held_ref, sems):
    tiles = order_ref.shape[1]
    tile = basis_ref.shape[0] // tiles
    step = 4
    copies = []
    for start in range(0, tiles, step):
        part = factor_rho * dot(
            basis_ref[pl.ds(start * tile, step * tile), :], returned_ref[...], 1, 1
        )
        held_ref[pl.ds(start * tile, step * tile), :] = part.astype(held_ref.dtype)
        for i in range(start, start + step):
            place = pl.multiple_of(order_ref[0, i] * tile, tile)
            copies.append(
                pltpu.make_async_copy(
                    held_ref.at[pl.ds(i * tile, tile), :],
                    out_ref.at[pl.ds(place, tile), :],
                    sems.at[i],
                )
            )
            copies[-1].start()
    for copy in copies:
        copy.wait()


def expand_rows(returned, basis, skeleton, factor_rho):
    columns, rank = returned.shape
    rows = basis.shape[0]
    tiles = skeleton.shape[1]

    def body(*refs):
        expand_kernel(factor_rho, *refs)

    return pl.pallas_call(
        body,
        name="expand",
        out_shape=jax.ShapeDtypeStruct((rows, columns), BF16),
        in_specs=[smem(), vmem(), vmem()],
        out_specs=hbm(),
        scratch_shapes=[pltpu.VMEM((rows, columns), BF16), pltpu.SemaphoreType.DMA((tiles,))],
        compiler_params=pltpu.CompilerParams(vmem_limit_bytes=VMEM_LIMIT),
        cost_estimate=cost(2 * rows * columns * rank, 2 * rows * (columns + rank)),
    )(skeleton, returned, basis)


def from_partner(array, axis, bit):
    return lax.ppermute(array, axis, [(i, i ^ 1 << bit) for i in range(lax.axis_size(axis))])


def shared_out(array, axis):
    count = lax.axis_size(axis)
    blocks = array.reshape(count, array.shape[0] // count, array.shape[1])
    return lax.all_to_all(blocks, axis, split_axis=0, concat_axis=0, tiled=True)


def times(left, right, right_dim):
    if left.dtype == BF16:
        return dot(left, right, 1, right_dim)
    return lax.dot_general(
        left,
        right.astype(F32),
        (((1,), (right_dim,)), ((), ())),
        precision=lax.Precision.HIGHEST,
        preferred_element_type=F32,
    )


def sent(array, level):
    return array.astype(BF16) if level >= 2 else array


def forward_levels(coefficient, factors):
    rank = factors.shape[1]
    for level in range(factors.shape[0]):
        partner = from_partner(sent(coefficient, level), "bfly", level)
        own = times(coefficient, factors[level, :, :rank], 1)
        coefficient = own + times(partner, factors[level, :, rank:], 1)
    return coefficient


def adjoint_levels(coefficient, factors):
    rank = factors.shape[1]
    for level in reversed(range(2, factors.shape[0])):
        sending = times(coefficient, factors[level, :, rank:], 0)
        received = from_partner(sent(sending, level), "bfly", level)
        coefficient = times(coefficient, factors[level, :, :rank], 0) + received.astype(F32)
    return coefficient


def swapped(array, mask):
    return lax.ppermute(array, "cblk", [(i, i ^ mask) for i in range(lax.axis_size("cblk"))])


def per_device(source, basis, transfer, skeleton, row_class, linear_table, cubic_table):
    factors = transfer[:, 0]
    rank = basis.shape[1]
    shares = lax.axis_size("cblk")
    factor_rho = math.sqrt(source.shape[0] * shares / rank)
    leaves, packed = leaf_terms(source, basis, skeleton, row_class)
    leaves = shared_out(leaves, "cblk")
    columns = leaves.shape[1]
    whole = jax.ShapeDtypeStruct((columns, rank), F32)
    fours = jax.ShapeDtypeStruct((4, columns, rank), BF16)
    eights = jax.ShapeDtypeStruct((shares, columns, rank), BF16)

    far = [swapped(packed, mask) for mask in range(2, shares, 2)]
    near = [swapped(packed, 1)]
    near += [swapped(array, 1) for array in far]
    extra = from_partner(factors[0, :, rank:], "bfly", 1)

    carried = forward_levels(leaves.astype(F32).sum(axis=0), factors).astype(BF16)
    back = middle(carried, [packed, *far, *near], linear_table, cubic_table, factor_rho)
    high = adjoint_levels(back, factors)
    send, own = small_call(down_send_kernel, (fours, whole), high, factors, extra)
    returned = small_call(down_take_kernel, eights, own, in_fours(send), factors)
    returned = lax.all_to_all(returned, "cblk", split_axis=0, concat_axis=0, tiled=True)
    return expand_rows(returned.reshape(shares * columns, rank), basis, skeleton, factor_rho)


def solution(mesh):
    placed = (
        P(("ens", "bfly", "cblk"), None),
        P(("ens", "bfly", "cblk"), None),
        P("ens", "bfly", None, None),
        P(("ens", "bfly", "cblk"), None),
        P(("ens", "bfly", "cblk")),
        P(),
        P(),
    )

    return jax.shard_map(
        per_device,
        mesh=mesh,
        in_specs=placed,
        out_specs=P(("ens", "bfly", "cblk"), None),
        check_vma=False,
    )
```

```python
import math

import jax
import jax.numpy as jnp
from jax import lax
from jax.experimental import pallas as pl
from jax.experimental.pallas import tpu as pltpu
from jax.sharding import PartitionSpec as P


F32 = jnp.float32
BF16 = jnp.bfloat16
VMEM_LIMIT = 24 * 1024 * 1024
LEAF_LIMIT = 65600000
LABEL_ROWS = 16


def vmem():
    return pl.BlockSpec(memory_space=pltpu.VMEM)


def hbm():
    return pl.BlockSpec(memory_space=pltpu.HBM)


def smem():
    return pl.BlockSpec(memory_space=pltpu.SMEM)


def cost(flops, bytes_accessed):
    return pl.CostEstimate(flops=flops, bytes_accessed=bytes_accessed, transcendentals=0)


def dot(left, right, left_dim, right_dim):
    return lax.dot_general(
        left, right, (((left_dim,), (right_dim,)), ((), ())), preferred_element_type=F32
    )


def leaf_kernel(
    order_hbm,
    class_hbm,
    source_hbm,
    basis_hbm,
    out_ref,
    acc_ref,
    order_ref,
    place_ref,
    class_ref,
    source_ref,
    basis_ref,
    sems,
    source_sems,
):
    rows = source_ref.shape[0]
    tiles = order_ref.shape[1]
    tile = rows // tiles
    shares = out_ref.shape[0]
    width = out_ref.shape[2]
    columns = source_ref.shape[1] // shares
    step = 4
    order_in = pltpu.make_async_copy(order_hbm, order_ref, sems.at[0])
    basis_in = pltpu.make_async_copy(basis_hbm, basis_ref, sems.at[1])
    source_in = [
        pltpu.make_async_copy(
            source_hbm.at[pl.ds(at * tile, step * tile), :],
            source_ref.at[pl.ds(at * tile, step * tile), :],
            source_sems.at[at // step],
        )
        for at in range(0, tiles, step)
    ]
    class_in = pltpu.make_async_copy(class_hbm, class_ref, sems.at[2])
    for copy in (order_in, class_in, basis_in, *source_in):
        copy.start()
    order_in.wait()
    for i in range(tiles):
        place_ref[order_ref[0, i]] = i
    class_in.wait()
    label = [class_ref[:, pl.ds(at, width)].astype(F32) for at in range(0, rows, width)]
    label.append(jnp.zeros((LABEL_ROWS - len(label), width), F32))
    label = jnp.concatenate(label, axis=0).astype(out_ref.dtype)
    for share in range(shares):
        out_ref[share, columns:, :] = label
    basis_in.wait()
    for start in range(0, tiles, step):
        source_in[start // step].wait()
        matched = jnp.concatenate(
            [
                basis_ref[pl.ds(pl.multiple_of(place_ref[start + i] * tile, tile), tile), :]
                for i in range(step)
            ],
            axis=0,
        )
        term = dot(source_ref[pl.ds(start * tile, step * tile), :], matched, 0, 0)
        if start == 0:
            acc_ref[...] = term
        elif start + step < tiles:
            acc_ref[...] += term
        else:
            total = (acc_ref[...] + term).astype(out_ref.dtype)
            for share in range(shares):
                out_ref[share, :columns, :] = total[share * columns : (share + 1) * columns]


def leaf_terms(source, basis, skeleton, row_class, shares):
    rows, columns = source.shape
    rank = basis.shape[1]
    return pl.pallas_call(
        leaf_kernel,
        name="leaf",
        out_shape=jax.ShapeDtypeStruct((shares, columns // shares + LABEL_ROWS, rank), BF16),
        in_specs=[hbm()] * 4,
        out_specs=vmem(),
        scratch_shapes=[
            pltpu.VMEM((columns, rank), F32),
            pltpu.SMEM(skeleton.shape, jnp.int32),
            pltpu.SMEM((skeleton.shape[1],), jnp.int32),
            pltpu.VMEM((1, rows), jnp.int32),
            pltpu.VMEM(source.shape, source.dtype),
            pltpu.VMEM(basis.shape, basis.dtype),
            pltpu.SemaphoreType.DMA((3,)),
            pltpu.SemaphoreType.DMA((skeleton.shape[1] // 4,)),
        ],
        compiler_params=pltpu.CompilerParams(vmem_limit_bytes=LEAF_LIMIT),
        cost_estimate=cost(2 * rows * columns * rank, 2 * rows * (columns + rank)),
    )(skeleton, row_class.reshape(1, rows), source, basis)


def product(left, right, right_dim):
    rows = left.shape[0]
    high = left.astype(BF16)
    low = (left - high.astype(F32)).astype(BF16)
    both = dot(jnp.concatenate([high, low], axis=0), right, 1, right_dim)
    return both[:rows] + both[rows:]


def factor(factors_ref, level, part):
    rank = factors_ref.shape[1]
    return factors_ref[level, :, part * rank : (part + 1) * rank]


def in_group():
    return lax.rem(lax.axis_index("bfly"), 4)


def spread(send_ref, first, second, third):
    place = in_group()
    send_ref[place] = first.astype(send_ref.dtype)
    send_ref[place ^ 1] = first.astype(send_ref.dtype)
    send_ref[place ^ 2] = second.astype(send_ref.dtype)
    send_ref[place ^ 3] = third.astype(send_ref.dtype)


def down_send_kernel(value_ref, factors_ref, extra_ref, send_ref, own_ref):
    value = value_ref[...]
    own = product(value, factor(factors_ref, 1, 0), 0)
    far = product(value, factor(factors_ref, 1, 1), 0)
    own_ref[...] = own
    spread(
        send_ref,
        product(own, factor(factors_ref, 0, 1), 0),
        far,
        product(far, extra_ref[...], 0),
    )


def down_take_kernel(own_ref, arrived_ref, factors_ref, out_ref):
    place = in_group()
    total = product(
        own_ref[...] + arrived_ref[place ^ 2].astype(F32), factor(factors_ref, 0, 0), 0
    )
    total += arrived_ref[place ^ 1].astype(F32) + arrived_ref[place ^ 3].astype(F32)
    out_ref[...] = jnp.broadcast_to(total.astype(out_ref.dtype), out_ref.shape)


def small_call(body, out_shape, *args):
    return pl.pallas_call(
        body,
        out_shape=out_shape,
        in_specs=[vmem()] * len(args),
        out_specs=jax.tree.map(lambda _: vmem(), out_shape),
        compiler_params=pltpu.CompilerParams(vmem_limit_bytes=VMEM_LIMIT),
        cost_estimate=cost(1 << 27, 1 << 20),
    )(*args)


def in_fours(array):
    size = lax.axis_size("bfly")
    groups = [list(range(start, start + 4)) for start in range(0, size, 4)]
    return lax.all_to_all(
        array, "bfly", split_axis=0, concat_axis=0, axis_index_groups=groups, tiled=True
    )


def in_three(table):
    high = table.astype(BF16)
    rest = table - high.astype(F32)
    middle = rest.astype(BF16)
    low = (rest - middle.astype(F32)).astype(BF16)
    return jnp.concatenate([high.astype(F32), middle.astype(F32), low.astype(F32)], axis=0)


def looked_kernel(rows, arrived_ref, linear_ref, cubic_ref, out_ref, table_ref):
    count, tall, width = arrived_ref.shape
    columns = tall - LABEL_ROWS
    classes = linear_ref.shape[0]
    lanes = table_ref.shape[1]
    shares = lanes // columns
    mine = lax.axis_index("cblk")
    wide = pl.ds(pl.multiple_of(mine // shares * lanes, lanes), lanes)
    share = pl.ds(pl.multiple_of(lax.rem(mine, shares) * columns, columns), columns)
    table_ref[0] = in_three(linear_ref[:, wide]).T
    table_ref[1] = in_three(cubic_ref[:, wide]).T
    tables = jnp.concatenate([table_ref[0, share, :], table_ref[1, share, :]], axis=0).astype(BF16)
    ids = lax.broadcasted_iota(jnp.int32, (classes, width), 0).astype(F32)
    for at in range(count):
        labels = arrived_ref[mine ^ at, columns:, :].astype(F32)
        for part in range(rows // width):
            hot = (ids == labels[part : part + 1]).astype(F32)
            hot = jnp.concatenate([hot, hot, hot], axis=0).astype(BF16)
            out_ref[:, pl.ds(at * rows + part * width, width)] = dot(tables, hot, 1, 0)


def looked_up(arrived, linear_table, cubic_table, rows):
    count, tall, _ = arrived.shape
    columns = tall - LABEL_ROWS

    def body(*refs):
        looked_kernel(rows, *refs)

    return pl.pallas_call(
        body,
        name="looked",
        out_shape=jax.ShapeDtypeStruct((2 * columns, count * rows), F32),
        in_specs=[vmem()] * 3,
        out_specs=vmem(),
        scratch_shapes=[pltpu.VMEM((2, max(columns, 128), 3 * linear_table.shape[0]), F32)],
        compiler_params=pltpu.CompilerParams(vmem_limit_bytes=VMEM_LIMIT),
        cost_estimate=cost(1 << 30, 1 << 23),
    )(arrived, linear_table, cubic_table)


def middle_kernel(factor_rho, carried_ref, looked_ref, *refs):
    bases, out_ref = refs[:-1], refs[-1]
    columns, width = carried_ref.shape
    rows = bases[0].shape[0]
    step = 2 * width
    total = jnp.zeros((columns, width), F32)
    for at, ref in enumerate(bases):
        for start in range(0, rows, step):
            basis = ref[pl.ds(start, step), :]
            mapped = factor_rho * dot(carried_ref[...], basis, 1, 1)
            here = pl.ds(at * rows + start, step)
            linear = looked_ref[:columns, here]
            cubic = looked_ref[columns:, here]
            weighted = mapped * (linear + cubic * mapped * mapped)
            total += dot(weighted.astype(BF16), basis, 1, 0)
    out_ref[...] = total


def middle(carried, looked, bases, factor_rho):
    columns, rank = carried.shape
    count = len(bases)
    rows = bases[0].shape[0]

    def body(*refs):
        middle_kernel(factor_rho, *refs)

    return pl.pallas_call(
        body,
        name="middle",
        out_shape=jax.ShapeDtypeStruct((columns, rank), F32),
        in_specs=[vmem()] * (2 + count),
        out_specs=vmem(),
        compiler_params=pltpu.CompilerParams(vmem_limit_bytes=VMEM_LIMIT),
        cost_estimate=cost(8 * count * rows * columns * rank, 2 * count * rows * rank),
    )(carried, looked, *bases)


def expand_kernel(factor_rho, order_ref, returned_ref, basis_ref, out_ref, held_ref, sems):
    tiles = order_ref.shape[1]
    tile = basis_ref.shape[0] // tiles
    step = 4
    copies = []
    for start in range(0, tiles, step):
        part = factor_rho * dot(
            basis_ref[pl.ds(start * tile, step * tile), :], returned_ref[...], 1, 1
        )
        held_ref[pl.ds(start * tile, step * tile), :] = part.astype(held_ref.dtype)
        for i in range(start, start + step):
            place = pl.multiple_of(order_ref[0, i] * tile, tile)
            copies.append(
                pltpu.make_async_copy(
                    held_ref.at[pl.ds(i * tile, tile), :],
                    out_ref.at[pl.ds(place, tile), :],
                    sems.at[i],
                )
            )
            copies[-1].start()
    for copy in copies:
        copy.wait()


def expand_rows(returned, basis, skeleton, factor_rho):
    columns, rank = returned.shape
    rows = basis.shape[0]
    tiles = skeleton.shape[1]

    def body(*refs):
        expand_kernel(factor_rho, *refs)

    return pl.pallas_call(
        body,
        name="expand",
        out_shape=jax.ShapeDtypeStruct((rows, columns), BF16),
        in_specs=[smem(), vmem(), vmem()],
        out_specs=hbm(),
        scratch_shapes=[pltpu.VMEM((rows, columns), BF16), pltpu.SemaphoreType.DMA((tiles,))],
        compiler_params=pltpu.CompilerParams(vmem_limit_bytes=VMEM_LIMIT),
        cost_estimate=cost(2 * rows * columns * rank, 2 * rows * (columns + rank)),
    )(skeleton, returned, basis)


def from_partner(array, axis, bit):
    return lax.ppermute(array, axis, [(i, i ^ 1 << bit) for i in range(lax.axis_size(axis))])


def times(left, right, right_dim):
    if left.dtype == BF16:
        return dot(left, right, 1, right_dim)
    return lax.dot_general(
        left,
        right.astype(F32),
        (((1,), (right_dim,)), ((), ())),
        precision=lax.Precision.HIGHEST,
        preferred_element_type=F32,
    )


def sent(array, level):
    return array.astype(BF16) if level >= 2 else array


def forward_levels(coefficient, factors):
    rank = factors.shape[1]
    for level in range(factors.shape[0]):
        partner = from_partner(sent(coefficient, level), "bfly", level)
        own = times(coefficient, factors[level, :, :rank], 1)
        coefficient = own + times(partner, factors[level, :, rank:], 1)
    return coefficient


def adjoint_levels(coefficient, factors):
    rank = factors.shape[1]
    for level in reversed(range(2, factors.shape[0])):
        sending = times(coefficient, factors[level, :, rank:], 0)
        received = from_partner(sent(sending, level), "bfly", level)
        coefficient = times(coefficient, factors[level, :, :rank], 0) + received.astype(F32)
    return coefficient


def swapped(array, mask):
    return lax.ppermute(array, "cblk", [(i, i ^ mask) for i in range(lax.axis_size("cblk"))])


def in_mask_order(basis, far, near):
    even = [basis, *far]
    return [array for pair in zip(even, near) for array in pair]


def per_device(source, basis, transfer, skeleton, row_class, linear_table, cubic_table):
    factors = transfer[:, 0]
    rank = basis.shape[1]
    shares = lax.axis_size("cblk")
    factor_rho = math.sqrt(source.shape[0] * shares / rank)
    columns = source.shape[1] // shares
    leaves = leaf_terms(source, basis, skeleton, row_class, shares)
    leaves = lax.all_to_all(leaves, "cblk", split_axis=0, concat_axis=0, tiled=True)
    whole = jax.ShapeDtypeStruct((columns, rank), F32)
    fours = jax.ShapeDtypeStruct((4, columns, rank), BF16)
    eights = jax.ShapeDtypeStruct((shares, columns, rank), BF16)

    far = [swapped(basis, mask) for mask in range(2, shares, 2)]
    near = [swapped(basis, 1)]
    near += [swapped(array, 1) for array in far]
    extra = from_partner(factors[0, :, rank:], "bfly", 1)
    looked = looked_up(leaves, linear_table, cubic_table, source.shape[0])

    summed = leaves[:, :columns].astype(F32).sum(axis=0)
    carried = forward_levels(summed, factors).astype(BF16)
    bases = in_mask_order(basis, far, near)
    back = middle(carried, looked, bases, factor_rho)
    high = adjoint_levels(back, factors)
    send, own = small_call(down_send_kernel, (fours, whole), high, factors, extra)
    returned = small_call(down_take_kernel, eights, own, in_fours(send), factors)
    returned = lax.all_to_all(returned, "cblk", split_axis=0, concat_axis=0, tiled=True)
    return expand_rows(returned.reshape(shares * columns, rank), basis, skeleton, factor_rho)


def solution(mesh):
    placed = (
        P(("ens", "bfly", "cblk"), None),
        P(("ens", "bfly", "cblk"), None),
        P("ens", "bfly", None, None),
        P(("ens", "bfly", "cblk"), None),
        P(("ens", "bfly", "cblk")),
        P(),
        P(),
    )

    return jax.shard_map(
        per_device,
        mesh=mesh,
        in_specs=placed,
        out_specs=P(("ens", "bfly", "cblk"), None),
        check_vma=False,
    )
```

```python
import math

import jax
import jax.numpy as jnp
from jax import lax
from jax.experimental import pallas as pl
from jax.experimental.pallas import tpu as pltpu
from jax.sharding import PartitionSpec as P


F32 = jnp.float32
BF16 = jnp.bfloat16
VMEM_LIMIT = 24 * 1024 * 1024
LEAF_LIMIT = 65600000
LABEL_ROWS = 16


def vmem():
    return pl.BlockSpec(memory_space=pltpu.VMEM)


def hbm():
    return pl.BlockSpec(memory_space=pltpu.HBM)


def smem():
    return pl.BlockSpec(memory_space=pltpu.SMEM)


def cost(flops, bytes_accessed):
    return pl.CostEstimate(flops=flops, bytes_accessed=bytes_accessed, transcendentals=0)


def dot(left, right, left_dim, right_dim):
    return lax.dot_general(
        left, right, (((left_dim,), (right_dim,)), ((), ())), preferred_element_type=F32
    )


def leaf_kernel(
    order_hbm,
    class_hbm,
    source_hbm,
    basis_hbm,
    out_ref,
    packed_hbm,
    acc_ref,
    order_ref,
    place_ref,
    class_ref,
    source_ref,
    basis_ref,
    label_ref,
    sems,
    source_sems,
):
    rows = source_ref.shape[0]
    tiles = order_ref.shape[1]
    tile = rows // tiles
    step = 4
    order_in = pltpu.make_async_copy(order_hbm, order_ref, sems.at[0])
    basis_in = pltpu.make_async_copy(basis_hbm, basis_ref, sems.at[1])
    source_in = [
        pltpu.make_async_copy(
            source_hbm.at[pl.ds(at * tile, step * tile), :],
            source_ref.at[pl.ds(at * tile, step * tile), :],
            source_sems.at[at // step],
        )
        for at in range(0, tiles, step)
    ]
    class_in = pltpu.make_async_copy(class_hbm, class_ref, sems.at[2])
    for copy in (order_in, basis_in, *source_in, class_in):
        copy.start()
    order_in.wait()
    for i in range(tiles):
        place_ref[order_ref[0, i]] = i
    basis_in.wait()
    basis_out = pltpu.make_async_copy(basis_ref, packed_hbm.at[pl.ds(0, rows), :], sems.at[3])
    basis_out.start()
    for start in range(0, tiles, step):
        source_in[start // step].wait()
        matched = jnp.concatenate(
            [
                basis_ref[pl.ds(pl.multiple_of(place_ref[start + i] * tile, tile), tile), :]
                for i in range(step)
            ],
            axis=0,
        )
        term = dot(source_ref[pl.ds(start * tile, step * tile), :], matched, 0, 0)
        if start == 0:
            acc_ref[...] = term
        elif start + step < tiles:
            acc_ref[...] += term
        else:
            out_ref[...] = (acc_ref[...] + term).astype(out_ref.dtype)
        if start == 0:
            class_in.wait()
            width = label_ref.shape[1]
            label = [class_ref[:, pl.ds(at, width)].astype(F32) for at in range(0, rows, width)]
            label.append(jnp.zeros((label_ref.shape[0] - len(label), width), F32))
            label_ref[...] = jnp.concatenate(label, axis=0).astype(label_ref.dtype)
        elif start == step:
            label_out = pltpu.make_async_copy(
                label_ref, packed_hbm.at[pl.ds(rows, label_ref.shape[0]), :], sems.at[4]
            )
            label_out.start()
    basis_out.wait()
    label_out.wait()


def leaf_terms(source, basis, skeleton, row_class):
    rows, columns = source.shape
    rank = basis.shape[1]
    labels = LABEL_ROWS
    return pl.pallas_call(
        leaf_kernel,
        name="leaf",
        out_shape=(
            jax.ShapeDtypeStruct((columns, rank), BF16),
            jax.ShapeDtypeStruct((rows + labels, rank), BF16),
        ),
        in_specs=[hbm()] * 4,
        out_specs=(vmem(), hbm()),
        scratch_shapes=[
            pltpu.VMEM((columns, rank), F32),
            pltpu.SMEM(skeleton.shape, jnp.int32),
            pltpu.SMEM((skeleton.shape[1],), jnp.int32),
            pltpu.VMEM((1, rows), jnp.int32),
            pltpu.VMEM(source.shape, source.dtype),
            pltpu.VMEM(basis.shape, basis.dtype),
            pltpu.VMEM((labels, rank), BF16),
            pltpu.SemaphoreType.DMA((5,)),
            pltpu.SemaphoreType.DMA((skeleton.shape[1] // 4,)),
        ],
        compiler_params=pltpu.CompilerParams(vmem_limit_bytes=LEAF_LIMIT),
        cost_estimate=cost(2 * rows * columns * rank, 2 * rows * (columns + rank)),
    )(skeleton, row_class.reshape(1, rows), source, basis)


def product(left, right, right_dim):
    rows = left.shape[0]
    high = left.astype(BF16)
    low = (left - high.astype(F32)).astype(BF16)
    both = dot(jnp.concatenate([high, low], axis=0), right, 1, right_dim)
    return both[:rows] + both[rows:]


def factor(factors_ref, level, part):
    rank = factors_ref.shape[1]
    return factors_ref[level, :, part * rank : (part + 1) * rank]


def in_group():
    return lax.rem(lax.axis_index("bfly"), 4)


def spread(send_ref, first, second, third):
    place = in_group()
    send_ref[place] = first.astype(send_ref.dtype)
    send_ref[place ^ 1] = first.astype(send_ref.dtype)
    send_ref[place ^ 2] = second.astype(send_ref.dtype)
    send_ref[place ^ 3] = third.astype(send_ref.dtype)


def down_send_kernel(value_ref, factors_ref, extra_ref, send_ref, own_ref):
    value = value_ref[...]
    own = product(value, factor(factors_ref, 1, 0), 0)
    far = product(value, factor(factors_ref, 1, 1), 0)
    own_ref[...] = own
    spread(
        send_ref,
        product(own, factor(factors_ref, 0, 1), 0),
        far,
        product(far, extra_ref[...], 0),
    )


def down_take_kernel(own_ref, arrived_ref, factors_ref, out_ref):
    place = in_group()
    total = product(
        own_ref[...] + arrived_ref[place ^ 2].astype(F32), factor(factors_ref, 0, 0), 0
    )
    total += arrived_ref[place ^ 1].astype(F32) + arrived_ref[place ^ 3].astype(F32)
    out_ref[...] = jnp.broadcast_to(total.astype(out_ref.dtype), out_ref.shape)


def small_call(body, out_shape, *args):
    return pl.pallas_call(
        body,
        out_shape=out_shape,
        in_specs=[vmem()] * len(args),
        out_specs=jax.tree.map(lambda _: vmem(), out_shape),
        compiler_params=pltpu.CompilerParams(vmem_limit_bytes=VMEM_LIMIT),
        cost_estimate=cost(1 << 27, 1 << 20),
    )(*args)


def in_fours(array):
    size = lax.axis_size("bfly")
    groups = [list(range(start, start + 4)) for start in range(0, size, 4)]
    return lax.all_to_all(
        array, "bfly", split_axis=0, concat_axis=0, axis_index_groups=groups, tiled=True
    )


def in_three(table):
    high = table.astype(BF16)
    rest = table - high.astype(F32)
    middle = rest.astype(BF16)
    low = (rest - middle.astype(F32)).astype(BF16)
    return jnp.concatenate([high.astype(F32), middle.astype(F32), low.astype(F32)], axis=0)


def hot_parts(labels, part, classes):
    ids = lax.broadcasted_iota(jnp.int32, (classes, labels.shape[1]), 0).astype(F32)
    hot = (ids == labels[part : part + 1]).astype(F32)
    return jnp.concatenate([hot, hot, hot], axis=0).astype(BF16)


def looked_kernel(linear_ref, cubic_ref, *refs):
    packed = refs[:-3]
    out_ref, parts_ref, table_ref = refs[-3:]
    columns = parts_ref.shape[0] // 2
    classes = linear_ref.shape[0]
    rows = packed[0].shape[0] - LABEL_ROWS
    width = packed[0].shape[1]
    lanes = table_ref.shape[1]
    shares = lanes // columns
    mine = lax.axis_index("cblk")
    wide = pl.ds(pl.multiple_of(mine // shares * lanes, lanes), lanes)
    share = pl.ds(pl.multiple_of(lax.rem(mine, shares) * columns, columns), columns)
    table_ref[0] = in_three(linear_ref[:, wide]).T
    table_ref[1] = in_three(cubic_ref[:, wide]).T
    tables = jnp.concatenate([table_ref[0, share, :], table_ref[1, share, :]], axis=0).astype(BF16)
    parts_ref[...] = tables
    for at, ref in enumerate(packed):
        labels = ref[pl.ds(rows, LABEL_ROWS), :].astype(F32)
        for part in range(rows // width):
            out_ref[:, pl.ds(at * rows + part * width, width)] = dot(
                tables, hot_parts(labels, part, classes), 1, 0
            )


def looked_up(packed, linear_table, cubic_table, columns):
    count = len(packed)
    rows = packed[0].shape[0] - LABEL_ROWS
    classes = linear_table.shape[0]
    return pl.pallas_call(
        looked_kernel,
        name="looked",
        out_shape=(
            jax.ShapeDtypeStruct((2 * columns, count * rows), F32),
            jax.ShapeDtypeStruct((2 * columns, 3 * classes), BF16),
        ),
        in_specs=[vmem()] * (2 + count),
        out_specs=(vmem(), vmem()),
        scratch_shapes=[pltpu.VMEM((2, max(columns, 128), 3 * classes), F32)],
        compiler_params=pltpu.CompilerParams(vmem_limit_bytes=VMEM_LIMIT),
        cost_estimate=cost(1 << 30, 1 << 23),
    )(linear_table, cubic_table, *packed)


def middle_kernel(factor_rho, early, carried_ref, looked_ref, parts_ref, *refs):
    packed, out_ref = refs[:-1], refs[-1]
    columns, width = carried_ref.shape
    classes = parts_ref.shape[1] // 3
    rows = packed[0].shape[0] - LABEL_ROWS
    step = 2 * width
    total = jnp.zeros((columns, width), F32)
    for at, ref in enumerate(packed):
        labels = ref[pl.ds(rows, LABEL_ROWS), :].astype(F32)
        for start in range(0, rows, step):
            basis = ref[pl.ds(start, step), :]
            mapped = factor_rho * dot(carried_ref[...], basis, 1, 1)
            if at < early:
                looked = looked_ref[:, pl.ds(at * rows + start, step)]
            else:
                first = start // width
                hot = [hot_parts(labels, first + i, classes) for i in range(2)]
                looked = dot(parts_ref[...], jnp.concatenate(hot, axis=1), 1, 0)
            weighted = mapped * (looked[:columns] + looked[columns:] * mapped * mapped)
            total += dot(weighted.astype(BF16), basis, 1, 0)
    out_ref[...] = total


def middle(carried, looked, parts, packed, early, factor_rho):
    columns, rank = carried.shape
    count = len(packed)
    tall = packed[0].shape[0]

    def body(*refs):
        middle_kernel(factor_rho, early, *refs)

    return pl.pallas_call(
        body,
        name="middle",
        out_shape=jax.ShapeDtypeStruct((columns, rank), F32),
        in_specs=[vmem()] * (3 + count),
        out_specs=vmem(),
        compiler_params=pltpu.CompilerParams(vmem_limit_bytes=VMEM_LIMIT),
        cost_estimate=cost(8 * count * tall * columns * rank, 2 * count * tall * rank),
    )(carried, looked, parts, *packed)


def expand_kernel(factor_rho, order_ref, returned_ref, basis_ref, out_ref, held_ref, sems):
    tiles = order_ref.shape[1]
    tile = basis_ref.shape[0] // tiles
    step = 4
    copies = []
    for start in range(0, tiles, step):
        part = factor_rho * dot(
            basis_ref[pl.ds(start * tile, step * tile), :], returned_ref[...], 1, 1
        )
        held_ref[pl.ds(start * tile, step * tile), :] = part.astype(held_ref.dtype)
        for i in range(start, start + step):
            place = pl.multiple_of(order_ref[0, i] * tile, tile)
            copies.append(
                pltpu.make_async_copy(
                    held_ref.at[pl.ds(i * tile, tile), :],
                    out_ref.at[pl.ds(place, tile), :],
                    sems.at[i],
                )
            )
            copies[-1].start()
    for copy in copies:
        copy.wait()


def expand_rows(returned, basis, skeleton, factor_rho):
    columns, rank = returned.shape
    rows = basis.shape[0]
    tiles = skeleton.shape[1]

    def body(*refs):
        expand_kernel(factor_rho, *refs)

    return pl.pallas_call(
        body,
        name="expand",
        out_shape=jax.ShapeDtypeStruct((rows, columns), BF16),
        in_specs=[smem(), vmem(), vmem()],
        out_specs=hbm(),
        scratch_shapes=[pltpu.VMEM((rows, columns), BF16), pltpu.SemaphoreType.DMA((tiles,))],
        compiler_params=pltpu.CompilerParams(vmem_limit_bytes=VMEM_LIMIT),
        cost_estimate=cost(2 * rows * columns * rank, 2 * rows * (columns + rank)),
    )(skeleton, returned, basis)


def from_partner(array, axis, bit):
    return lax.ppermute(array, axis, [(i, i ^ 1 << bit) for i in range(lax.axis_size(axis))])


def shared_out(array, axis):
    count = lax.axis_size(axis)
    blocks = array.reshape(count, array.shape[0] // count, array.shape[1])
    return lax.all_to_all(blocks, axis, split_axis=0, concat_axis=0, tiled=True)


def times(left, right, right_dim):
    if left.dtype == BF16:
        return dot(left, right, 1, right_dim)
    return lax.dot_general(
        left,
        right.astype(F32),
        (((1,), (right_dim,)), ((), ())),
        precision=lax.Precision.HIGHEST,
        preferred_element_type=F32,
    )


def sent(array, level):
    return array.astype(BF16) if level >= 2 else array


def forward_levels(coefficient, factors):
    rank = factors.shape[1]
    for level in range(factors.shape[0]):
        partner = from_partner(sent(coefficient, level), "bfly", level)
        own = times(coefficient, factors[level, :, :rank], 1)
        coefficient = own + times(partner, factors[level, :, rank:], 1)
    return coefficient


def adjoint_levels(value, factors):
    rank = factors.shape[1]
    sending = times(value, factors[-1, :, rank:], 0)
    for level in reversed(range(2, factors.shape[0])):
        received = from_partner(sent(sending, level), "bfly", level)
        own = times(value, factors[level, :, :rank], 0)
        if level > 2:
            ready = lax.optimization_barrier(times(own, factors[level - 1, :, rank:], 0))
            sending = ready + times(received, factors[level - 1, :, rank:], 0)
        value = own + received.astype(F32)
    return value


def swapped(array, mask):
    return lax.ppermute(array, "cblk", [(i, i ^ mask) for i in range(lax.axis_size("cblk"))])


def per_device(source, basis, transfer, skeleton, row_class, linear_table, cubic_table):
    factors = transfer[:, 0]
    rank = basis.shape[1]
    shares = lax.axis_size("cblk")
    factor_rho = math.sqrt(source.shape[0] * shares / rank)
    leaves, packed = leaf_terms(source, basis, skeleton, row_class)
    leaves = shared_out(leaves, "cblk")
    columns = leaves.shape[1]
    whole = jax.ShapeDtypeStruct((columns, rank), F32)
    fours = jax.ShapeDtypeStruct((4, columns, rank), BF16)
    eights = jax.ShapeDtypeStruct((shares, columns, rank), BF16)

    far = [swapped(packed, mask) for mask in range(2, shares, 2)]
    near = swapped(packed, 1)
    cross = [swapped(array, 1) for array in far]
    extra = from_partner(factors[0, :, rank:], "bfly", 1)
    early = [packed, near, *far]
    looked, parts = looked_up(early, linear_table, cubic_table, columns)

    carried = forward_levels(leaves.astype(F32).sum(axis=0), factors).astype(BF16)
    back = middle(carried, looked, parts, early + cross, len(early), factor_rho)
    high = adjoint_levels(back, factors)
    send, own = small_call(down_send_kernel, (fours, whole), high, factors, extra)
    returned = small_call(down_take_kernel, eights, own, in_fours(send), factors)
    returned = lax.all_to_all(returned, "cblk", split_axis=0, concat_axis=0, tiled=True)
    return expand_rows(returned.reshape(shares * columns, rank), basis, skeleton, factor_rho)


def solution(mesh):
    placed = (
        P(("ens", "bfly", "cblk"), None),
        P(("ens", "bfly", "cblk"), None),
        P("ens", "bfly", None, None),
        P(("ens", "bfly", "cblk"), None),
        P(("ens", "bfly", "cblk")),
        P(),
        P(),
    )

    return jax.shard_map(
        per_device,
        mesh=mesh,
        in_specs=placed,
        out_specs=P(("ens", "bfly", "cblk"), None),
        check_vma=False,
    )
```
